256 devices in a mesh: groups: 2 (over z), seq: 16 (over y, core), dp: 8 (over x).
Axes of the slice: x: 8, y: 8, z: 2, core: 2. Of those that a mesh axis runs over, the one named last changes fastest.
The devices are a block of a 8x8x16 slice.
Arguments:
- resid: bfloat16 [16, 1024, 2048], P(('groups', 'dp'), 'seq'), parts along dimension 0, may hold values from -6 to 6
- queries_keys: bfloat16 [2, 16, 1024, 2048], P(None, ('groups', 'dp'), 'seq'), parts along dimension 1, may hold values from -20 to 20
- values: bfloat16 [16, 1024, 2048], P(('groups', 'dp'), 'seq'), parts along dimension 0, may hold values from -6 to 6
- doc_ids: int32 [16, 1024], P(('groups', 'dp')), parts along dimension 0, may hold values from 0 to 5, never falling along the last dimension, each value on 1 to 512 neighbouring positions
- out_weight: bfloat16 [2048, 2048], P(None, 'dp'), may hold values from -0.125 to 0.125
- norm_gain: float32 [2048], replicated, may hold values from 0.5 to 1.5
- expert_ids: int32 [16, 1024, 4], P(('groups', 'dp'), 'seq'), parts along dimension 0, may hold values from 0 to 31, all different within a row; in each aligned block of 64 rows (0 to 63, 64 to 127, ..., all dimensions but the last counted through in order) at most 10 rows name the same one
- gate_vals: float32 [16, 1024, 4], P(('groups', 'dp'), 'seq'), parts along dimension 0, may hold values from 0.05 to 0.6
- expert_gate: bfloat16 [128, 2048, 352], P(('seq', 'dp')), may hold values from -0.125 to 0.125
- expert_up: bfloat16 [128, 2048, 352], P(('seq', 'dp')), may hold values from -0.125 to 0.125
- expert_down: bfloat16 [128, 352, 2048], P(('seq', 'dp')), may hold values from -0.15625 to 0.15625
- shared_gate: bfloat16 [2048, 2816], P(None, 'dp'), may hold values from -0.125 to 0.125
- shared_up: bfloat16 [2048, 2816], P(None, 'dp'), may hold values from -0.125 to 0.125
- shared_down: bfloat16 [2816, 2048], P('dp'), may hold values from -0.109375 to 0.109375
- shared_score: bfloat16 [2048], replicated, may hold values from -0.125 to 0.125
Outputs:
- layer_out: bfloat16 [16, 1024, 2048], P(('groups', 'dp'), 'seq'), parts along dimension 0
The draws below stay inside these ranges and needn't reach their ends.
There are 2 independent parts, one for each index of `groups`. The reference program is written for one: setup_inputs(seed, part) draws one part's arguments, and reference() takes and returns one part's arrays. A program takes and returns all parts, laid end to end along the dimension named above; an argument that names none is the same for every part. Nothing has to cross between parts.
Inputs may be any that keep to these rules, and one draw needn't show every extreme that they name: `doc_ids`: document numbers never fall along a sequence; each document holds 1 to 512 positions. `expert_ids`: each token names 4 different experts; among the rows of one device no expert is named more than 10 times.
All inputs are finite; a program needn't handle non-finite values.
Results may differ from the reference program's by a relative error of at most 0.01.
Values may be sent and summed in bfloat16 or wider, within the bound.
No kernel may reach another device: no remote copies, remote signals or barrier semaphores. Data moves between devices by JAX's collectives and lax.ppermute only.
A program may use at most 128 MiB of HBM per device.

```python
import math
import jax
import jax.numpy as jnp
import numpy as np
from jax import lax

HEADS = 16
HD = 128
D = 2048
EXPERTS = 32
TOPK = 4
FF_E = 1408
SPLIT = 4
PIECES = 128
PIECE_FF = 352
SH_FF = 2816
TOK_DEV = 64
CAP = 10
LENGTH = 1024
SEQS = 8
N_DP = 8


def draw_queries_keys(key, part):
    baseline = jnp.clip(jax.random.normal(key, (2, SEQS, LENGTH, D), jnp.float32), -6.0, 6.0)
    return baseline.astype(jnp.bfloat16)


def block_levels(rng, extent, pieces, smallest, largest):
    factor_of, own = 1.0, jax.random.fold_in(rng, 6)
    for dim, shards_of in pieces:
        heights = jnp.exp(jax.random.uniform(jax.random.fold_in(own, dim), (shards_of,), jnp.float32, smallest / len(pieces), largest / len(pieces)))
        factor_of = factor_of * jnp.repeat(heights, extent[dim] // shards_of).reshape([-1 if axis == dim else 1 for axis in range(len(extent))])
    return factor_of


def length_profile(number_of, total, reach, skew):
    loads = [(1 << 20) // math.isqrt(grade ** skew) + 1 for grade in range(2, number_of + 1)]
    rest, counts = total - reach - (number_of - 1), [1] * (number_of - 1)
    while rest > 0:
        candidates = [i for i in range(number_of - 1) if counts[i] < reach]
        mass, left = sum([loads[i] for i in candidates]), rest
        for i in candidates:
            addition = min(reach - counts[i], max(1, left * loads[i] // mass), rest)
            counts[i] = counts[i] + addition
            rest = rest - addition
    return np.array([reach] + counts)


def uneven_parts(rng, number_of, total, limit, slope):
    if number_of == 2:
        one = jax.random.randint(rng, (), max(1, total - limit), min(limit, total - 1) + 1)
        return jnp.stack([one, total - one])
    lengths = jnp.asarray(length_profile(number_of, total, limit, slope), jnp.int32)
    couples = (number_of - 1) // 2
    giver, taker = lengths[1:1 + 2 * couples:2], lengths[2:2 + 2 * couples:2]
    margin = jnp.minimum(giver - 1, limit - taker)
    moved = jax.random.randint(jax.random.fold_in(rng, 1), (couples,), 0, 1 << 20) % (margin + 1)
    lengths = lengths.at[1:1 + 2 * couples:2].set(giver - moved).at[2:2 + 2 * couples:2].set(taker + moved)
    return lengths[jax.random.permutation(jax.random.fold_in(rng, 2), number_of)]


def assign_block(own_key, own, number, rows, count, top, bound, skew):
    ranking = jax.random.permutation(own_key, count)
    heavy_load, common = shares(count, rows * top, bound, skew, True), shares(count, rows * top, bound, skew, False)
    places = jnp.arange(count)

    def named(lengths, turn):
        used = int((lengths > 0).sum())
        fixed = max(1, used // 4)
        moved = fixed + (places - fixed + turn * (used - fixed)) % max(1, count - fixed)
        return jnp.zeros((count,), jnp.int32).at[ranking[jnp.where(places < fixed, places, moved)]].set(jnp.asarray(lengths, jnp.int32))

    lengths = jnp.where(number % 4 == 0, named(heavy_load, number // 4), named(common, number - number // 4 - 1))
    mixed = jax.random.permutation(jax.random.fold_in(own, 3), count)
    giver, sink = mixed[0:count // 2 * 2:2], mixed[1:count // 2 * 2:2]
    room = jnp.minimum(lengths[giver] - 1, bound - lengths[sink]) // 2
    room = jnp.where((giver == ranking[0]) | (sink == ranking[0]) | (lengths[sink] == 0), 0, jnp.maximum(room, 0))
    moved = jax.random.randint(jax.random.fold_in(own, 4), (count // 2,), 0, 1 << 20) % (room + 1)
    lengths = lengths.at[giver].add(-moved).at[sink].add(moved)
    labels = jnp.searchsorted(jnp.cumsum(lengths), jnp.arange(rows * top), side="right").astype(jnp.int32)
    grid = labels.reshape(top, rows).T
    grid = grid[jax.random.permutation(jax.random.fold_in(own, 1), rows)]
    turn = jax.random.randint(jax.random.fold_in(own, 2), (rows, 1), 0, top)
    return jnp.take_along_axis(grid, (jnp.arange(top)[None, :] + turn) % top, axis=1)


def shares(number_of, total, bound, lean, full):
    weights = [(1 << 20) // math.isqrt(grade ** lean) + 1 for grade in range(1, number_of + 1)]
    largest = bound if full else min(bound, max(-(-total // number_of), total * weights[0] // sum(weights)))
    least = 1 if total - largest >= number_of - 1 else 0
    counts, rest = [largest] + [least] * (number_of - 1), total - largest - least * (number_of - 1)
    while rest > 0:
        free = [i for i in range(1, number_of) if counts[i] < largest] or [i for i in range(1, number_of) if counts[i] < bound]
        whole, budget = sum([weights[i] for i in free]), rest
        for i in free:
            more = min(bound - counts[i], max(1, budget * weights[i] // whole), rest)
            counts[i] = counts[i] + more
            rest = rest - more
    return np.array(counts)


def bell_draw(own_key, shape, scale, most, pieces=(), kind=jnp.bfloat16):
    gain = block_levels(own_key, shape, pieces, -0.22, 0.18) if pieces else 1.0
    values = jax.random.normal(own_key, shape, jnp.float32) * scale * gain
    return jnp.minimum(jnp.maximum(values, -most), most).astype(kind)


def setup_inputs(seed: int = 0, part: int = 0) -> dict:
    key_of = jax.random.split(jax.random.key(seed), 16)
    part_splits = jax.random.split(jax.random.fold_in(key_of[15], part), 16)
    resid = bell_draw(part_splits[0], (SEQS, LENGTH, D), 1.0, 6.0, ((0, 8), (1, 16)))
    queries_keys = draw_queries_keys(jax.random.fold_in(jax.random.fold_in(key_of[15], part), 71), part)
    values = bell_draw(part_splits[2], (SEQS, LENGTH, D), 1.0, 6.0, ((0, 8), (1, 16)))
    doc_ids = jax.vmap(lambda own: jnp.searchsorted(jnp.cumsum(uneven_parts(own, 6, LENGTH, LENGTH // 2, 1)), jnp.arange(LENGTH), side="right"))(jax.random.split(part_splits[3], SEQS)).reshape((SEQS, LENGTH)).astype(jnp.int32)
    out_weight = bell_draw(key_of[4], (D, D), D ** -0.5, 0.125, ((1, 8),))
    norm_gain = jnp.clip(1.0 + 0.1 * jax.random.normal(key_of[5], (D,), jnp.float32), 0.5, 1.5)
    expert_ids_keys = jax.random.split(jax.random.fold_in(part_splits[6], 1), SEQS * LENGTH // TOK_DEV)
    expert_ids_turns = jax.random.permutation(jax.random.fold_in(part_splits[6], 3), SEQS * LENGTH // TOK_DEV)
    expert_ids = jax.vmap(lambda own, number: assign_block(jax.random.fold_in(part_splits[6], 2), own, number, TOK_DEV, EXPERTS, TOPK, CAP, 2))(expert_ids_keys, expert_ids_turns).reshape((SEQS, LENGTH, TOPK))
    gate_vals = jnp.clip(jnp.exp(math.log(0.6) - 2.4849067 * jax.random.uniform(part_splits[7], (SEQS, LENGTH, TOPK), jnp.float32) ** block_levels(part_splits[7], (SEQS, LENGTH, TOPK), ((0, 8), (1, 16)), -0.2, 0.2)), 0.05, 0.6)
    expert_gate = bell_draw(key_of[8], (PIECES, D, PIECE_FF), D ** -0.5, 0.125, ((0, 128),))
    expert_up = bell_draw(key_of[9], (PIECES, D, PIECE_FF), D ** -0.5, 0.125, ((0, 128),))
    expert_down = bell_draw(key_of[10], (PIECES, PIECE_FF, D), FF_E ** -0.5, 0.15625, ((0, 128),))
    shared_gate = bell_draw(key_of[11], (D, SH_FF), D ** -0.5, 0.125, ((1, 8),))
    shared_up = bell_draw(key_of[12], (D, SH_FF), D ** -0.5, 0.125, ((1, 8),))
    shared_down = bell_draw(key_of[13], (SH_FF, D), SH_FF ** -0.5, 0.109375, ((0, 8),))
    shared_score = bell_draw(key_of[14], (D,), D ** -0.5, 0.125)
    return dict(resid=resid, queries_keys=queries_keys, values=values, doc_ids=doc_ids, out_weight=out_weight, norm_gain=norm_gain, expert_ids=expert_ids, gate_vals=gate_vals, expert_gate=expert_gate, expert_up=expert_up, expert_down=expert_down, shared_gate=shared_gate, shared_up=shared_up, shared_down=shared_down, shared_score=shared_score)


norm_eps = 1e-06

def slot_numbers(routes):
    flat_routes = routes.reshape(routes.shape[:-2] + (-1,))
    matches = (flat_routes[..., None] == jnp.arange(EXPERTS, dtype=jnp.int32)).astype(jnp.int32)
    ranked = lax.optimization_barrier(jnp.sum(matches * (jnp.cumsum(matches, axis=-2) - 1), axis=-1))
    return (flat_routes * CAP + ranked).reshape(routes.shape).astype(jnp.int32)

def reference(resid, queries_keys, values, doc_ids, out_weight, norm_gain, expert_ids, gate_vals, expert_gate, expert_up, expert_down, shared_gate, shared_up, shared_down, shared_score):
    score_scale = 1.0 / math.sqrt(HD)
    positions = jnp.arange(LENGTH, dtype=jnp.int32)
    causal = positions[:, None] >= positions[None, :]

    def attend_sequence(inputs):
        pair_rows, value_rows, documents = inputs
        queries = pair_rows[0].astype(jnp.float32).reshape(LENGTH, HEADS, HD)
        key_rows = pair_rows[1].astype(jnp.float32).reshape(LENGTH, HEADS, HD)
        value_heads = value_rows.astype(jnp.float32).reshape(LENGTH, HEADS, HD)
        scores = jnp.einsum('qhd,khd->hqk', queries, key_rows) * score_scale
        allowed = causal & (documents[:, None] == documents[None, :])
        scores = jnp.where(allowed[None], scores, -1e+30)
        row_max = lax.optimization_barrier(jnp.max(scores, axis=-1, keepdims=True))
        lifted = jnp.exp(scores - row_max)
        weights = (lifted / lax.optimization_barrier(jnp.sum(lifted, axis=-1, keepdims=True))).astype(jnp.bfloat16)
        attended = jnp.einsum('hqk,khd->qhd', weights.astype(jnp.float32), value_heads).astype(jnp.bfloat16)
        return jnp.dot(attended.reshape(LENGTH, D), out_weight, preferred_element_type=jnp.float32).astype(jnp.bfloat16)
    projected = lax.map(attend_sequence, (jnp.moveaxis(queries_keys, 1, 0), values, doc_ids))
    residual = (resid.astype(jnp.float32) + projected.astype(jnp.float32)).astype(jnp.bfloat16)
    stream = residual.astype(jnp.float32)
    normed = (stream * lax.rsqrt(lax.optimization_barrier(jnp.mean(stream * stream, axis=-1, keepdims=True)) + norm_eps) * norm_gain).astype(jnp.bfloat16)
    shared_width = SH_FF // N_DP
    down_blocks = shared_down.astype(jnp.float32).reshape(N_DP, shared_width, D)

    def shared_sequence(row_block):
        gate_act = jnp.dot(row_block, shared_gate, preferred_element_type=jnp.float32)
        up_act = jnp.dot(row_block, shared_up, preferred_element_type=jnp.float32)
        hidden = (jax.nn.silu(gate_act) * up_act).astype(jnp.bfloat16)
        partial_sums = jnp.einsum('lnf,nfd->nld', hidden.astype(jnp.float32).reshape(-1, N_DP, shared_width), down_blocks)
        partial_sums = lax.optimization_barrier(partial_sums.astype(jnp.bfloat16)).astype(jnp.float32)
        return lax.optimization_barrier(jnp.sum(partial_sums, axis=0))
    shared_out = lax.map(shared_sequence, normed).reshape(-1, D)
    flat_rows = normed.reshape(-1, D)
    token_count = flat_rows.shape[0]
    share_weight = jax.nn.sigmoid(jnp.dot(flat_rows, shared_score, preferred_element_type=jnp.float32))
    blocks = token_count // TOK_DEV
    routes = expert_ids.reshape(blocks, TOK_DEV, TOPK).astype(jnp.int32)
    slot_ids = slot_numbers(routes)
    ranked = slot_ids - routes * CAP
    block_ids = jnp.arange(blocks, dtype=jnp.int32)[:, None, None]
    token_ids = block_ids * TOK_DEV + jnp.arange(TOK_DEV, dtype=jnp.int32)[None, :, None] + jnp.zeros_like(routes)
    row_slots = (block_ids * CAP + ranked).astype(jnp.int32)
    row_table = jnp.full((EXPERTS, blocks * CAP), token_count, jnp.int32).at[routes, row_slots].set(token_ids.astype(jnp.int32))
    gate_table = jnp.zeros((EXPERTS, blocks * CAP), jnp.float32).at[routes, row_slots].set(gate_vals.reshape(blocks, TOK_DEV, TOPK).astype(jnp.float32))
    padded = jnp.concatenate([flat_rows, jnp.zeros((1, D), jnp.bfloat16)], axis=0)
    gate_pieces = expert_gate.reshape(EXPERTS, SPLIT, D, PIECE_FF)
    up_pieces = expert_up.reshape(EXPERTS, SPLIT, D, PIECE_FF)
    down_pieces = expert_down.reshape(EXPERTS, SPLIT, PIECE_FF, D)

    def one_expert(running, inputs):
        index_rows, weight_rows, gate_matrix, up_matrix, down_matrix = inputs
        picked = padded[index_rows].astype(jnp.float32)
        gate_act = jnp.einsum('rd,sdf->srf', picked, gate_matrix.astype(jnp.float32))
        up_act = jnp.einsum('rd,sdf->srf', picked, up_matrix.astype(jnp.float32))
        hidden = (jax.nn.silu(gate_act) * up_act).astype(jnp.bfloat16)
        partial_sums = jnp.einsum('srf,sfd->srd', hidden.astype(jnp.float32), down_matrix.astype(jnp.float32))
        partial_sums = lax.optimization_barrier(partial_sums.astype(jnp.bfloat16)).astype(jnp.float32)
        output = lax.optimization_barrier(jnp.sum(partial_sums, axis=0))
        running = running.at[index_rows].add(weight_rows[:, None] * output)
        return (running, None)
    routed, unused = lax.scan(one_expert, jnp.zeros((token_count + 1, D), jnp.float32), (row_table, gate_table, gate_pieces, up_pieces, down_pieces))
    routed = routed[:token_count]
    layer_out = residual.reshape(-1, D).astype(jnp.float32) + routed + share_weight[:, None] * shared_out
    return layer_out.astype(jnp.bfloat16).reshape(SEQS, LENGTH, D)
```

```python
import math

import jax
import jax.numpy as jnp
from jax import lax
from jax.sharding import PartitionSpec as P

HD = 128
EXPERTS = 32
TOPK = 4
SPLIT = 4
CAP = 10
PAIR = 2
META_ROWS = 16


norm_eps = 1e-06


def attend_heads(queries, key_rows, value_rows, documents):
    score_scale = 1.0 / math.sqrt(queries.shape[-1])
    scores = (
        lax.dot_general(
            queries, key_rows, (((1,), (1,)), ((), ())), preferred_element_type=jnp.float32
        )
        * score_scale
    )
    positions = jnp.arange(queries.shape[0], dtype=jnp.int32)
    allowed = (positions[:, None] >= positions[None, :]) & (
        documents[:, None] == documents[None, :]
    )
    scores = jnp.where(allowed, scores, -1e30)
    row_max = jnp.max(scores, axis=-1, keepdims=True)
    lifted = jnp.exp(scores - row_max)
    weights = (lifted / jnp.sum(lifted, axis=-1, keepdims=True)).astype(jnp.bfloat16)
    return jnp.dot(weights, value_rows, preferred_element_type=jnp.float32).astype(jnp.bfloat16)


def hidden_of(rows, gate_matrix, up_matrix):
    gate_act = jnp.dot(rows, gate_matrix, preferred_element_type=jnp.float32)
    up_act = jnp.dot(rows, up_matrix, preferred_element_type=jnp.float32)
    return (jax.nn.silu(gate_act) * up_act).astype(jnp.bfloat16)


def body(
    resid,
    queries_keys,
    values,
    doc_ids,
    out_weight,
    norm_gain,
    expert_ids,
    gate_vals,
    expert_gate,
    expert_up,
    expert_down,
    shared_gate,
    shared_up,
    shared_down,
    shared_score,
):
    seq_count = lax.axis_size("seq")
    batch_count = lax.axis_size("dp")
    seq_index = lax.axis_index("seq")
    batch_index = lax.axis_index("dp")
    tokens = resid.shape[1]
    model_width = resid.shape[2]
    columns = out_weight.shape[1]
    head_rows = model_width // seq_count
    experts_here = EXPERTS // seq_count

    packed = jnp.concatenate([queries_keys[:, 0], values], axis=0)
    packed = packed.reshape(3, tokens, seq_count, head_rows).transpose(2, 0, 1, 3)
    heads = lax.all_to_all(packed, "seq", split_axis=0, concat_axis=0, tiled=True)
    queries = heads[:, 0].reshape(seq_count * tokens, head_rows)
    key_rows = heads[:, 1].reshape(seq_count * tokens, head_rows)
    value_rows = heads[:, 2].reshape(seq_count * tokens, head_rows)

    own_rows = lax.dynamic_slice_in_dim(out_weight, seq_index * head_rows, head_rows, axis=0)
    routes_meta = jnp.stack(
        [expert_ids.reshape(-1).astype(jnp.bfloat16), gate_vals.reshape(-1).astype(jnp.bfloat16)]
    )
    meta = jnp.pad(routes_meta, ((0, META_ROWS - 2), (0, 0)))
    gathered = lax.all_gather(jnp.concatenate([own_rows, meta], axis=0), "dp", axis=0)
    head_weight = gathered[:, :head_rows].transpose(1, 0, 2).reshape(head_rows, model_width)
    full_weight = lax.all_gather(head_weight, "seq", axis=0, tiled=True)

    swap = [(i, i ^ 1) for i in range(batch_count)]
    other_gate = lax.ppermute(expert_gate[0], "dp", swap)
    other_up = lax.ppermute(expert_up[0], "dp", swap)

    attended = attend_heads(queries, key_rows, value_rows, doc_ids[0])
    own_attended = lax.all_to_all(
        attended.reshape(seq_count, tokens, head_rows), "seq", split_axis=0, concat_axis=0, tiled=True
    )
    own_attended = own_attended.transpose(1, 0, 2).reshape(tokens, model_width)
    projected = jnp.dot(own_attended, full_weight, preferred_element_type=jnp.float32).astype(
        jnp.bfloat16
    )
    residual = (resid[0].astype(jnp.float32) + projected.astype(jnp.float32)).astype(jnp.bfloat16)
    stream = residual.astype(jnp.float32)
    normed = (
        stream * lax.rsqrt(jnp.mean(stream * stream, axis=-1, keepdims=True) + norm_eps) * norm_gain
    ).astype(jnp.bfloat16)

    all_tokens = lax.all_gather(normed, "dp", axis=0, tiled=True)
    down_late, all_tokens = lax.optimization_barrier((expert_down[0], all_tokens))
    other_down = lax.ppermute(down_late, "dp", swap)

    flat = tokens * TOPK
    routes = gathered[:, head_rows].astype(jnp.int32).reshape(batch_count, flat)
    gates = gathered[:, head_rows + 1].reshape(batch_count, flat)
    order = jnp.arange(flat, dtype=jnp.int32)
    earlier = (routes[:, :, None] == routes[:, None, :]) & (order[None, :, None] > order[None, None, :])
    ranked = jnp.sum(earlier.astype(jnp.int32), axis=-1)
    served = batch_count // PAIR
    first = (batch_index % PAIR) * served
    place = jnp.arange(batch_count, dtype=jnp.int32)[:, None] - first
    mine = (
        (routes % experts_here == batch_index // SPLIT) & (place >= 0) & (place < served)
    )
    rows_each = served * CAP
    slot = jnp.where(
        mine, (routes // experts_here) * rows_each + place * CAP + ranked, -1
    ).reshape(batch_count * tokens, TOPK)
    total_rows = seq_count * rows_each
    row_range = jnp.arange(total_rows, dtype=jnp.int32)
    gate_rows = gates.reshape(batch_count * tokens, TOPK)
    picked = sum(
        [(slot[None, :, k] == row_range[:, None]).astype(jnp.bfloat16) for k in range(TOPK)]
    )
    combine = sum(
        [
            jnp.where(slot[:, k, None] == row_range[None, :], gate_rows[:, k, None], 0)
            for k in range(TOPK)
        ]
    ).astype(jnp.bfloat16)

    outgoing = jnp.dot(picked, all_tokens, preferred_element_type=jnp.float32).astype(jnp.bfloat16)
    incoming = lax.all_to_all(
        outgoing.reshape(seq_count, rows_each, model_width),
        "seq",
        split_axis=0,
        concat_axis=0,
        tiled=True,
    ).reshape(total_rows, model_width)

    shared_hidden = hidden_of(all_tokens, shared_gate, shared_up)
    share_weight = jax.nn.sigmoid(
        jnp.dot(all_tokens, shared_score, preferred_element_type=jnp.float32)
    )
    shared_part = (
        jnp.dot(shared_hidden, shared_down, preferred_element_type=jnp.float32)
        * share_weight[:, None]
    )

    results = (
        jnp.dot(
            hidden_of(incoming, expert_gate[0], expert_up[0]),
            expert_down[0],
            preferred_element_type=jnp.float32,
        )
        + jnp.dot(
            hidden_of(incoming, other_gate, other_up),
            other_down,
            preferred_element_type=jnp.float32,
        )
    ).astype(jnp.bfloat16)
    returned = lax.all_to_all(
        results.reshape(seq_count, rows_each, model_width),
        "seq",
        split_axis=0,
        concat_axis=0,
        tiled=True,
    ).reshape(total_rows, model_width)
    parts = (
        jnp.dot(combine, returned, preferred_element_type=jnp.float32) + shared_part
    ).astype(jnp.bfloat16)
    summed = lax.psum_scatter(parts, "dp", scatter_dimension=0, tiled=True)
    layer_out = residual.astype(jnp.float32) + summed.astype(jnp.float32)
    return layer_out.astype(jnp.bfloat16)[None]


def solution(mesh):
    placed = (
        P(("groups", "dp"), "seq", None),
        P(None, ("groups", "dp"), "seq", None),
        P(("groups", "dp"), "seq", None),
        P(("groups", "dp"), None),
        P(None, "dp"),
        P(),
        P(("groups", "dp"), "seq", None),
        P(("groups", "dp"), "seq", None),
        P(("seq", "dp"), None, None),
        P(("seq", "dp"), None, None),
        P(("seq", "dp"), None, None),
        P(None, "dp"),
        P(None, "dp"),
        P("dp", None),
        P(),
    )
    return jax.shard_map(
        body,
        mesh=mesh,
        in_specs=placed,
        out_specs=P(("groups", "dp"), "seq", None),
        check_vma=False,
    )
```

```python
import math

import jax
import jax.numpy as jnp
from jax import lax
from jax.sharding import PartitionSpec as P

HD = 128
EXPERTS = 32
TOPK = 4
SPLIT = 4
CAP = 10
PAIR = 2
CORES = 2
META_ROWS = 16
CHUNKS = 4
PROJ_CHUNKS = 2


norm_eps = 1e-06
f32 = jnp.float32
bf16 = jnp.bfloat16


def dot(a, b):
    return jnp.dot(a, b, preferred_element_type=f32)


def attend_heads(queries, key_rows, value_rows, documents):
    score_scale = 1.0 / math.sqrt(queries.shape[-1])
    scores = (
        lax.dot_general(queries, key_rows, (((1,), (1,)), ((), ())), preferred_element_type=f32)
        * score_scale
    )
    positions = jnp.arange(queries.shape[0], dtype=jnp.int32)
    allowed = (positions[:, None] >= positions[None, :]) & (
        documents[:, None] == documents[None, :]
    )
    scores = jnp.where(allowed, scores, -1e30)
    row_max = jnp.max(scores, axis=-1, keepdims=True)
    lifted = jnp.exp(scores - row_max)
    weights = (lifted / jnp.sum(lifted, axis=-1, keepdims=True)).astype(bf16)
    return dot(weights, value_rows).astype(bf16)


def ring_pairs(size, step):
    return [(i, (i + step) % size) for i in range(size)]


def ring_gather(block, axis, size, step):
    ahead, behind = ring_pairs(size, -step), ring_pairs(size, step)
    count = size // step
    found = {0: block}
    for hop in range(1, count // 2 + 1):
        found[hop] = lax.ppermute(found[hop - 1], axis, ahead)
        if hop < count - count // 2:
            found[count - hop] = lax.ppermute(found[(count - hop + 1) % count], axis, behind)
    return [found[j] for j in range(count)]


def ring_scatter(parts, axis, size, step):
    forward, backward = ring_pairs(size, step), ring_pairs(size, -step)
    count = size // step
    half = count // 2
    left = parts[half].astype(bf16)
    right = parts[half - 1].astype(bf16)
    for hop in range(1, half + 1):
        left = lax.ppermute(left, axis, backward)
        if hop < half:
            left = (left.astype(f32) + parts[half + hop].astype(f32)).astype(bf16)
        if hop < half:
            right = lax.ppermute(right, axis, forward)
            if hop < half - 1:
                right = (right.astype(f32) + parts[half - 1 - hop].astype(f32)).astype(bf16)
    return parts[0].astype(f32) + left.astype(f32) + right.astype(f32)


def body(
    resid,
    queries_keys,
    values,
    doc_ids,
    out_weight,
    norm_gain,
    expert_ids,
    gate_vals,
    expert_gate,
    expert_up,
    expert_down,
    shared_gate,
    shared_up,
    shared_down,
    shared_score,
):
    seq_count = lax.axis_size("seq")
    batch_count = lax.axis_size("dp")
    seq_index = lax.axis_index("seq")
    batch_index = lax.axis_index("dp")
    tokens = resid.shape[1]
    model_width = resid.shape[2]
    head_rows = model_width // seq_count
    experts_here = EXPERTS // seq_count
    chips = seq_count // CORES

    with jax.named_scope("heads"):
        packed = jnp.concatenate([queries_keys[:, 0], values], axis=0)
        packed = packed.reshape(3, tokens, seq_count, head_rows).transpose(2, 0, 1, 3)
        heads = lax.all_to_all(packed, "seq", split_axis=0, concat_axis=0, tiled=True)
    queries = heads[:, 0].reshape(seq_count * tokens, head_rows)
    key_rows = heads[:, 1].reshape(seq_count * tokens, head_rows)
    value_rows = heads[:, 2].reshape(seq_count * tokens, head_rows)

    with jax.named_scope("rows"):
        own_rows = lax.dynamic_slice_in_dim(out_weight, seq_index * head_rows, head_rows, axis=0)
        routes_meta = jnp.stack(
            [expert_ids.reshape(-1).astype(bf16), gate_vals.reshape(-1).astype(bf16)]
        )
        meta = jnp.pad(routes_meta, ((0, META_ROWS - 2), (0, 0)))
        spread = jnp.broadcast_to(
            jnp.concatenate([own_rows, meta], axis=0)[None],
            (batch_count, head_rows + META_ROWS, out_weight.shape[1]),
        )
        gathered = lax.all_to_all(spread, "dp", split_axis=0, concat_axis=0, tiled=True)
    head_weight = gathered[:, :head_rows].transpose(1, 0, 2).reshape(head_rows, model_width)

    swap = [(i, i ^ 1) for i in range(batch_count)]
    with jax.named_scope("trade_gate"):
        other_gate = lax.ppermute(expert_gate[0], "dp", swap)
    with jax.named_scope("trade_up"):
        other_up = lax.ppermute(expert_up[0], "dp", swap)
    with jax.named_scope("trade_down"):
        other_down = lax.ppermute(expert_down[0], "dp", swap)

    with jax.named_scope("attend"):
        attended = attend_heads(queries, key_rows, value_rows, doc_ids[0])

    with jax.named_scope("project"):
        core = seq_index % CORES
        blocks = attended.reshape(chips, CORES * tokens * head_rows)
        blocks = lax.dynamic_slice_in_dim(
            jnp.concatenate([blocks, blocks], axis=0), seq_index // CORES, chips, axis=0
        ).reshape(chips, CORES, tokens, head_rows)
        own_blocks = lax.dynamic_index_in_dim(blocks, core, axis=1, keepdims=False)
        partner_blocks = lax.dynamic_index_in_dim(blocks, 1 - core, axis=1, keepdims=False)
        own_blocks = own_blocks.reshape(chips * tokens, head_rows)
        partner_blocks = partner_blocks.reshape(chips * tokens, head_rows)
        cores = [(i, i ^ 1) for i in range(seq_count)]
        width = model_width // PROJ_CHUNKS
        pieces = []
        for part in range(PROJ_CHUNKS):
            weight = head_weight[:, part * width : (part + 1) * width]
            crossed = lax.ppermute(dot(partner_blocks, weight).astype(bf16), "seq", cores)
            both = dot(own_blocks, weight) + crossed.astype(f32)
            both = both.reshape(chips, tokens, width)
            pieces.append(
                ring_scatter([both[j] for j in range(chips)], "seq", seq_count, CORES)
            )
        projected = jnp.concatenate(pieces, axis=1).astype(bf16)
    residual = (resid[0].astype(f32) + projected.astype(f32)).astype(bf16)
    stream = residual.astype(f32)
    normed = (
        stream * lax.rsqrt(jnp.mean(stream * stream, axis=-1, keepdims=True) + norm_eps) * norm_gain
    ).astype(bf16)

    flat = tokens * TOPK
    routes_gates = gathered[:, head_rows : head_rows + 2]
    routes_gates = lax.dynamic_slice_in_dim(
        jnp.concatenate([routes_gates, routes_gates], axis=0), batch_index, batch_count, axis=0
    )
    routes = routes_gates[:, 0].astype(jnp.int32)
    order = jnp.arange(flat, dtype=jnp.int32)
    earlier = (routes[:, :, None] == routes[:, None, :]) & (order[None, :, None] > order[None, None, :])
    ranked = jnp.sum(earlier.astype(jnp.int32), axis=-1)
    served = batch_count // PAIR
    ahead = jnp.arange(batch_count, dtype=jnp.int32)[:, None]
    place = jnp.where(batch_index % 2 == 0, (batch_count - ahead) % batch_count, ahead)
    mine = (routes % experts_here == batch_index // SPLIT) & (place < served)
    rows_each = served * CAP
    slot = jnp.where(
        mine, (routes // experts_here) * rows_each + place * CAP + ranked, -1
    ).reshape(batch_count * tokens, TOPK)
    total_rows = seq_count * rows_each
    row_range = jnp.arange(total_rows, dtype=jnp.int32)
    gate_rows = routes_gates[:, 1].reshape(batch_count * tokens, TOPK)
    picked = sum([(slot[None, :, k] == row_range[:, None]).astype(bf16) for k in range(TOPK)])
    combine = sum(
        [
            jnp.where(slot[:, k, None] == row_range[None, :], gate_rows[:, k, None], 0)
            for k in range(TOPK)
        ]
    ).astype(bf16)
    picked, combine = lax.optimization_barrier((picked, combine))

    chunk = model_width // CHUNKS
    cuts = [slice(c * chunk, (c + 1) * chunk) for c in range(CHUNKS)]
    sums = [0.0] * 4
    shared_sums = [0.0] * 2
    scored = 0.0
    all_tokens = None
    earlier_rows = []
    for c, cut in enumerate(cuts):
        with jax.named_scope(f"gather_{c}"):
            block = normed[:, cut]
            if c == 1:
                block, all_tokens = lax.optimization_barrier((block, all_tokens))
            if c > 1:
                block, all_tokens, earlier_rows[c - 2] = lax.optimization_barrier(
                    (block, all_tokens, earlier_rows[c - 2])
                )
            all_tokens = jnp.concatenate(ring_gather(block, "dp", batch_count, 1), axis=0)
        with jax.named_scope(f"send_{c}"):
            outgoing = dot(picked, all_tokens).astype(bf16)
            incoming = lax.all_to_all(
                outgoing.reshape(seq_count, rows_each, chunk),
                "seq",
                split_axis=0,
                concat_axis=0,
                tiled=True,
            ).reshape(total_rows, chunk)
            earlier_rows.append(incoming)
        with jax.named_scope(f"expert_in_{c}"):
            matrices = (expert_gate[0], expert_up[0], other_gate, other_up)
            sums = [s + dot(incoming, m[cut]) for s, m in zip(sums, matrices)]
        with jax.named_scope(f"shared_in_{c}"):
            shared_sums = [
                s + dot(all_tokens, m[cut]) for s, m in zip(shared_sums, (shared_gate, shared_up))
            ]
            scored = scored + dot(all_tokens, shared_score[cut])

    share_weight = jax.nn.sigmoid(scored)
    shared_hidden = (jax.nn.silu(shared_sums[0]) * shared_sums[1]).astype(bf16)
    own_hidden = (jax.nn.silu(sums[0]) * sums[1]).astype(bf16)
    other_hidden = (jax.nn.silu(sums[2]) * sums[3]).astype(bf16)
    outs = []
    for c, cut in enumerate(cuts):
        with jax.named_scope(f"expert_out_{c}"):
            results = (
                dot(own_hidden, expert_down[0][:, cut]) + dot(other_hidden, other_down[:, cut])
            ).astype(bf16)
        with jax.named_scope(f"return_{c}"):
            returned = lax.all_to_all(
                results.reshape(seq_count, rows_each, chunk),
                "seq",
                split_axis=0,
                concat_axis=0,
                tiled=True,
            ).reshape(total_rows, chunk)
        with jax.named_scope(f"shared_out_{c}"):
            shared_part = dot(shared_hidden, shared_down[:, cut]) * share_weight[:, None]
        with jax.named_scope(f"combine_{c}"):
            parts = dot(combine, returned) + shared_part
            if c:
                parts, outs[-1] = lax.optimization_barrier((parts, outs[-1]))
            parts = parts.reshape(batch_count, tokens, chunk)
            outs.append(
                ring_scatter([parts[j] for j in range(batch_count)], "dp", batch_count, 1)
            )
    layer_out = residual.astype(f32) + jnp.concatenate(outs, axis=1)
    return layer_out.astype(bf16)[None]


def solution(mesh):
    placed = (
        P(("groups", "dp"), "seq", None),
        P(None, ("groups", "dp"), "seq", None),
        P(("groups", "dp"), "seq", None),
        P(("groups", "dp"), None),
        P(None, "dp"),
        P(),
        P(("groups", "dp"), "seq", None),
        P(("groups", "dp"), "seq", None),
        P(("seq", "dp"), None, None),
        P(("seq", "dp"), None, None),
        P(("seq", "dp"), None, None),
        P(None, "dp"),
        P(None, "dp"),
        P("dp", None),
        P(),
    )
    return jax.shard_map(
        body,
        mesh=mesh,
        in_specs=placed,
        out_specs=P(("groups", "dp"), "seq", None),
        check_vma=False,
    )
```

```python
import math

import jax
import jax.numpy as jnp
from jax import lax
from jax.sharding import PartitionSpec as P


EXPERTS = 32
TOPK = 4
SPLIT = 4
CAP = 10
PAIR = 2
CORES = 2
META_ROWS = 16
BATCHES = 2
PROJ_CHUNKS = 2
HALVES = 2


norm_eps = 1e-06
f32 = jnp.float32
bf16 = jnp.bfloat16


def dot(a, b):
    return jnp.dot(a, b, preferred_element_type=f32)


def attend_heads(queries, key_rows, value_rows, documents):
    score_scale = 1.0 / math.sqrt(queries.shape[-1])
    scores = (
        lax.dot_general(queries, key_rows, (((1,), (1,)), ((), ())), preferred_element_type=f32)
        * score_scale
    )
    positions = jnp.arange(queries.shape[0], dtype=jnp.int32)
    allowed = (positions[:, None] >= positions[None, :]) & (
        documents[:, None] == documents[None, :]
    )
    scores = jnp.where(allowed, scores, -1e30)
    row_max = jnp.max(scores, axis=-1, keepdims=True)
    lifted = jnp.exp(scores - row_max)
    weights = (lifted / jnp.sum(lifted, axis=-1, keepdims=True)).astype(bf16)
    return dot(weights, value_rows).astype(bf16)


def hidden_of(rows, gate_matrix, up_matrix):
    return (jax.nn.silu(dot(rows, gate_matrix)) * dot(rows, up_matrix)).astype(bf16)


def ring_pairs(size, step):
    return [(i, (i + step) % size) for i in range(size)]


def ring_scatter(parts, axis, size, step):
    forward, backward = ring_pairs(size, step), ring_pairs(size, -step)
    count = size // step
    half = count // 2
    left = parts[half].astype(bf16)
    right = parts[half - 1].astype(bf16)
    for hop in range(1, half + 1):
        left = lax.ppermute(left, axis, backward)
        if hop < half:
            left = (left.astype(f32) + parts[half + hop].astype(f32)).astype(bf16)
        if hop < half:
            right = lax.ppermute(right, axis, forward)
            if hop < half - 1:
                right = (right.astype(f32) + parts[half - 1 - hop].astype(f32)).astype(bf16)
    return parts[0].astype(f32) + left.astype(f32) + right.astype(f32)


def layer(
    resid,
    queries_keys,
    values,
    doc_ids,
    out_weight,
    norm_gain,
    expert_ids,
    gate_vals,
    expert_gate,
    expert_up,
    expert_down,
    shared_gate,
    shared_up,
    shared_down,
    shared_score,
):
    seq_count = lax.axis_size("seq")
    batch_count = lax.axis_size("dp")
    seq_index = lax.axis_index("seq")
    batch_index = lax.axis_index("dp")
    tokens = resid.shape[1]
    model_width = resid.shape[2]
    head_rows = model_width // seq_count
    experts_here = EXPERTS // seq_count
    chips = seq_count // CORES

    packed = jnp.concatenate([queries_keys[:, 0], values], axis=0)
    packed = packed.reshape(3, tokens, seq_count, head_rows).transpose(2, 0, 1, 3)
    heads = lax.all_to_all(packed, "seq", split_axis=0, concat_axis=0, tiled=True)
    queries = heads[:, 0].reshape(seq_count * tokens, head_rows)
    key_rows = heads[:, 1].reshape(seq_count * tokens, head_rows)
    value_rows = heads[:, 2].reshape(seq_count * tokens, head_rows)

    own_rows = lax.dynamic_slice_in_dim(out_weight, seq_index * head_rows, head_rows, axis=0)
    routes_meta = jnp.stack(
        [expert_ids.reshape(-1).astype(bf16), gate_vals.reshape(-1).astype(bf16)]
    )
    meta = jnp.pad(routes_meta, ((0, META_ROWS - 2), (0, 0)))
    gathered = lax.all_gather(jnp.concatenate([own_rows, meta], axis=0), "dp", axis=0)
    swap = [(i, i ^ 1) for i in range(batch_count)]
    own_gate, gathered = lax.optimization_barrier((expert_gate[0], gathered))
    other_gate = lax.ppermute(own_gate, "dp", swap)
    head_weight = gathered[:, :head_rows].transpose(1, 0, 2).reshape(head_rows, model_width)
    rolled_meta = gathered[:, head_rows : head_rows + 2]
    rolled_meta = lax.dynamic_slice_in_dim(
        jnp.concatenate([rolled_meta, rolled_meta], axis=0), batch_index, batch_count, axis=0
    )

    attended = attend_heads(queries, key_rows, value_rows, doc_ids[0])

    core = seq_index % CORES
    blocks = attended.reshape(chips, CORES * tokens * head_rows)
    blocks = lax.dynamic_slice_in_dim(
        jnp.concatenate([blocks, blocks], axis=0), seq_index // CORES, chips, axis=0
    ).reshape(chips, CORES, tokens, head_rows)
    own_blocks = lax.dynamic_index_in_dim(blocks, core, axis=1, keepdims=False)
    partner_blocks = lax.dynamic_index_in_dim(blocks, 1 - core, axis=1, keepdims=False)
    own_blocks = own_blocks.reshape(chips * tokens, head_rows)
    partner_blocks = partner_blocks.reshape(chips * tokens, head_rows)
    cores = [(i, i ^ 1) for i in range(seq_count)]
    width = model_width // PROJ_CHUNKS
    pieces = []
    for part in range(PROJ_CHUNKS):
        weight = head_weight[:, part * width : (part + 1) * width]
        crossed = lax.ppermute(dot(partner_blocks, weight).astype(bf16), "seq", cores)
        both = dot(own_blocks, weight) + crossed.astype(f32)
        both = both.reshape(chips, tokens, width)
        pieces.append(
            ring_scatter([both[j] for j in range(chips)], "seq", seq_count, CORES)
        )
    projected = jnp.concatenate(pieces, axis=1).astype(bf16)
    residual = (resid[0].astype(f32) + projected.astype(f32)).astype(bf16)
    stream = residual.astype(f32)
    normed = (
        stream * lax.rsqrt(jnp.mean(stream * stream, axis=-1, keepdims=True) + norm_eps) * norm_gain
    ).astype(bf16)

    even = batch_index % 2 == 0
    flat = tokens * TOPK
    served = batch_count // PAIR
    per_batch = served // BATCHES
    batch_tokens = per_batch * tokens
    routes_gates = jnp.stack(
        [rolled_meta[0]]
        + [
            jnp.where(even, rolled_meta[batch_count - hop], rolled_meta[hop])
            for hop in range(1, served)
        ]
    )
    routes = routes_gates[:, 0].astype(jnp.int32)
    order = jnp.arange(flat, dtype=jnp.int32)
    earlier = (routes[:, :, None] == routes[:, None, :]) & (order[None, :, None] > order[None, None, :])
    ranked = jnp.sum(earlier.astype(jnp.int32), axis=-1)
    place = jnp.arange(served, dtype=jnp.int32)[:, None] % per_batch
    rows_each = per_batch * CAP
    block_rows = HALVES * rows_each
    half_width = model_width // HALVES
    slot = jnp.where(
        routes % experts_here == batch_index // SPLIT,
        (routes // experts_here) * block_rows + place * CAP + ranked,
        -block_rows,
    ).reshape(served * tokens, TOPK)
    batch_rows = seq_count * rows_each
    row_range = jnp.arange(HALVES * batch_rows, dtype=jnp.int32)
    gate_rows = routes_gates[:, 1].reshape(served * tokens, TOPK)
    picks, combines = [], []
    for batch in range(BATCHES):
        span = slice(batch * batch_tokens, (batch + 1) * batch_tokens)
        places = jnp.concatenate([slot[span] + h * rows_each for h in range(HALVES)], axis=0)
        gate_two = jnp.concatenate([gate_rows[span]] * HALVES, axis=0)
        picks.append(
            sum([(places[None, :, k] == row_range[:, None]).astype(bf16) for k in range(TOPK)])
        )
        combines.append(
            sum(
                [
                    jnp.where(places[:, k, None] == row_range[None, :], gate_two[:, k, None], 0)
                    for k in range(TOPK)
                ]
            ).astype(bf16)
        )
    by_device = row_range // block_rows * rows_each + row_range % rows_each
    by_half = row_range // rows_each % HALVES * batch_rows + by_device
    to_half = (by_half[None, :] == row_range[:, None]).astype(bf16)
    to_device = (by_half[:, None] == row_range[None, :]).astype(bf16)
    picks, combines, to_half, to_device = lax.optimization_barrier(
        (picks, combines, to_half, to_device)
    )

    half = batch_count // 2
    ahead, behind = {0: normed}, {0: normed}
    for hop in range(1, half):
        ahead[hop] = lax.ppermute(ahead[hop - 1], "dp", ring_pairs(batch_count, -1))
        behind[hop] = lax.ppermute(behind[hop - 1], "dp", ring_pairs(batch_count, 1))
    ahead[half] = lax.ppermute(ahead[half - 1], "dp", ring_pairs(batch_count, -1))
    mine = [normed] + [jnp.where(even, behind[hop], ahead[hop]) for hop in range(1, served)]
    all_tokens = jnp.concatenate(
        [ahead[j] for j in range(half + 1)] + [behind[j] for j in range(half - 1, 0, -1)], axis=0
    )
    own_up, own_down, ahead[half] = lax.optimization_barrier(
        (expert_up[0], expert_down[0], ahead[half])
    )
    other_up = lax.ppermute(own_up, "dp", swap)
    other_down = lax.ppermute(own_down, "dp", swap)

    def stack_halves(rows):
        return jnp.concatenate(
            [rows[:, h * half_width : (h + 1) * half_width] for h in range(HALVES)], axis=0
        )

    def along_seq(rows):
        return lax.all_to_all(
            rows.reshape(seq_count, block_rows, half_width),
            "seq",
            split_axis=0,
            concat_axis=0,
            tiled=True,
        ).reshape(HALVES * batch_rows, half_width)

    incoming = []
    for batch in range(BATCHES):
        block = jnp.concatenate(mine[batch * per_batch : (batch + 1) * per_batch], axis=0)
        outgoing = dot(picks[batch], stack_halves(block)).astype(bf16)
        if batch:
            outgoing, incoming[-1] = lax.optimization_barrier((outgoing, incoming[-1]))
        incoming.append(along_seq(outgoing))

    share_weight = jax.nn.sigmoid(dot(all_tokens, shared_score))
    shared_part = dot(hidden_of(all_tokens, shared_gate, shared_up), shared_down)
    shared_part = (shared_part * share_weight[:, None]).astype(bf16)

    shared_part, incoming[-1] = lax.optimization_barrier((shared_part, incoming[-1]))
    shared_part = shared_part.reshape(batch_count, tokens, model_width).astype(f32)
    results = []
    for batch in range(BATCHES):
        rows = dot(to_half, incoming[batch]).astype(bf16)
        rows = jnp.concatenate(
            [rows[h * batch_rows : (h + 1) * batch_rows] for h in range(HALVES)], axis=1
        )
        out = (
            dot(hidden_of(rows, expert_gate[0], expert_up[0]), expert_down[0])
            + dot(hidden_of(rows, other_gate, other_up), other_down)
        ).astype(bf16)
        results.append(dot(to_device, stack_halves(out)).astype(bf16))

    routed = [None] * served
    last = None
    for batch in reversed(range(BATCHES)):
        rows = results[batch]
        if last is not None:
            rows, last = lax.optimization_barrier((rows, last))
        last = along_seq(rows)
        parts = dot(combines[batch], last).reshape(HALVES, per_batch, tokens, half_width)
        for i in range(per_batch):
            routed[batch * per_batch + i] = jnp.concatenate(
                [parts[h, i] for h in range(HALVES)], axis=1
            )

    def part_behind(hop):
        return shared_part[batch_count - hop] + jnp.where(even, routed[hop], 0.0)

    def part_ahead(hop):
        return shared_part[hop] + jnp.where(even, 0.0, routed[hop])

    back = shared_part[half].astype(bf16)
    forth = part_ahead(half - 1).astype(bf16)
    for hop in range(half - 1, -1, -1):
        back = lax.ppermute(back, "dp", ring_pairs(batch_count, -1))
        if hop:
            back = (back.astype(f32) + part_behind(hop)).astype(bf16)
            forth = lax.ppermute(forth, "dp", ring_pairs(batch_count, 1))
        if hop > 1:
            forth = (forth.astype(f32) + part_ahead(hop - 1)).astype(bf16)
    layer_out = (
        residual.astype(f32)
        + routed[0]
        + shared_part[0]
        + back.astype(f32)
        + forth.astype(f32)
    )
    return layer_out.astype(bf16)[None]


def solution(mesh):
    placed = (
        P(("groups", "dp"), "seq", None),
        P(None, ("groups", "dp"), "seq", None),
        P(("groups", "dp"), "seq", None),
        P(("groups", "dp"), None),
        P(None, "dp"),
        P(),
        P(("groups", "dp"), "seq", None),
        P(("groups", "dp"), "seq", None),
        P(("seq", "dp"), None, None),
        P(("seq", "dp"), None, None),
        P(("seq", "dp"), None, None),
        P(None, "dp"),
        P(None, "dp"),
        P("dp", None),
        P(),
    )
    return jax.shard_map(
        layer,
        mesh=mesh,
        in_specs=placed,
        out_specs=P(("groups", "dp"), "seq", None),
        check_vma=False,
    )
```

```python
import math

import jax
import jax.numpy as jnp
from jax import lax
from jax.experimental import pallas as pl
from jax.experimental.pallas import tpu as pltpu
from jax.sharding import PartitionSpec as P


EXPERTS = 32
TOPK = 4
SPLIT = 4
CAP = 10
PAIR = 2
CORES = 2
META_ROWS = 16
BATCHES = 2
PROJ_CHUNKS = 2
HALVES = 2
STEPS = 2


norm_eps = 1e-06
f32 = jnp.float32
bf16 = jnp.bfloat16


def dot(a, b):
    return jnp.dot(a, b, preferred_element_type=f32)


def attend_heads(queries, key_rows, value_rows, documents):
    score_scale = 1.0 / math.sqrt(queries.shape[-1])
    scores = (
        lax.dot_general(queries, key_rows, (((1,), (1,)), ((), ())), preferred_element_type=f32)
        * score_scale
    )
    positions = jnp.arange(queries.shape[0], dtype=jnp.int32)
    allowed = (positions[:, None] >= positions[None, :]) & (
        documents[:, None] == documents[None, :]
    )
    scores = jnp.where(allowed, scores, -1e30)
    row_max = jnp.max(scores, axis=-1, keepdims=True)
    lifted = jnp.exp(scores - row_max)
    weights = (lifted / jnp.sum(lifted, axis=-1, keepdims=True)).astype(bf16)
    return dot(weights, value_rows).astype(bf16)


def hidden_of(rows, gate_matrix, up_matrix):
    return (jax.nn.silu(dot(rows, gate_matrix)) * dot(rows, up_matrix)).astype(bf16)


def expert_kernel(x, to_half, to_device, go, uo, do, gx, ux, dx, y, rows, sums):
    step = pl.program_id(0)
    count, width = rows.shape[0], x.shape[1]

    @pl.when(step == 0)
    def _():
        for h in range(HALVES):
            rows[:, h * width : (h + 1) * width] = dot(
                to_half[h * count : (h + 1) * count, :], x[...]
            ).astype(bf16)

    def across(a, b):
        return lax.dot_general(a, b, (((1,), (1,)), ((), ())), preferred_element_type=f32)

    part = None
    for g, u, d in ((go, uo, do), (gx, ux, dx)):
        gate_act = across(rows[...], g[...])
        up_act = across(rows[...], u[...])
        hidden = (gate_act / (1.0 + jnp.exp(-gate_act)) * up_act).astype(bf16)
        out = dot(hidden, d[...])
        part = out if part is None else part + out

    @pl.when(step == 0)
    def _():
        sums[...] = part

    @pl.when(step > 0)
    def _():
        sums[...] = sums[...] + part

    @pl.when(step == pl.num_programs(0) - 1)
    def _():
        total = None
        for h in range(HALVES):
            out = sums[:, h * width : (h + 1) * width].astype(bf16)
            term = dot(to_device[:, h * count : (h + 1) * count], out)
            total = term if total is None else total + term
        y[...] = total.astype(bf16)


def expert_blocks(x, to_half, to_device, own, other):
    hidden, model_width = own[0].shape
    tile = hidden // STEPS
    count = x.shape[0] // HALVES
    whole = [pl.BlockSpec(a.shape, lambda j: (0, 0)) for a in (x, to_half, to_device)]
    tiled = [pl.BlockSpec((tile, model_width), lambda j: (j, 0))] * 6
    return pl.pallas_call(
        expert_kernel,
        grid=(STEPS,),
        in_specs=whole + tiled,
        out_specs=pl.BlockSpec(x.shape, lambda j: (0, 0)),
        out_shape=jax.ShapeDtypeStruct(x.shape, bf16),
        scratch_shapes=[
            pltpu.VMEM((count, model_width), bf16),
            pltpu.VMEM((count, model_width), f32),
        ],
        compiler_params=pltpu.CompilerParams(
            dimension_semantics=("arbitrary",), vmem_limit_bytes=60 << 20
        ),
        cost_estimate=pl.CostEstimate(
            flops=12 * count * hidden * model_width,
            bytes_accessed=12 * hidden * model_width,
            transcendentals=2 * count * hidden,
        ),
        name="expert_blocks",
    )(x, to_half, to_device, *own, *other)


def columns_kernel(starts, *refs):
    blocks, out = refs[:-1], refs[-1]
    width = blocks[0].shape[1]
    for j, block in enumerate(blocks):
        start = pl.multiple_of(starts[j], width)
        out[:, pl.ds(start, width)] = block[: out.shape[0], :]


def columns_in_order(blocks, first, rows):
    count, width = len(blocks), blocks[0].shape[1]
    starts = (first + jnp.arange(count, dtype=jnp.int32)) % count * width
    return pl.pallas_call(
        columns_kernel,
        in_specs=[pl.BlockSpec(memory_space=pltpu.SMEM)]
        + [pl.BlockSpec(memory_space=pltpu.VMEM)] * count,
        out_specs=pl.BlockSpec(memory_space=pltpu.VMEM),
        out_shape=jax.ShapeDtypeStruct((rows, count * width), bf16),
        name="columns_in_order",
    )(starts, *blocks)


def ring_pairs(size, step):
    return [(i, (i + step) % size) for i in range(size)]


def ring_scatter(parts, axis, size, step):
    forward, backward = ring_pairs(size, step), ring_pairs(size, -step)
    count = size // step
    half = count // 2
    left = parts[half].astype(bf16)
    right = parts[half - 1].astype(bf16)
    for hop in range(1, half + 1):
        left = lax.ppermute(left, axis, backward)
        if hop < half:
            left = (left.astype(f32) + parts[half + hop].astype(f32)).astype(bf16)
        if hop < half:
            right = lax.ppermute(right, axis, forward)
            if hop < half - 1:
                right = (right.astype(f32) + parts[half - 1 - hop].astype(f32)).astype(bf16)
    return parts[0].astype(f32) + left.astype(f32) + right.astype(f32)


def layer(
    resid,
    queries_keys,
    values,
    doc_ids,
    out_weight,
    norm_gain,
    expert_ids,
    gate_vals,
    expert_gate,
    expert_up,
    expert_down,
    shared_gate,
    shared_up,
    shared_down,
    shared_score,
):
    seq_count = lax.axis_size("seq")
    batch_count = lax.axis_size("dp")
    seq_index = lax.axis_index("seq")
    batch_index = lax.axis_index("dp")
    tokens = resid.shape[1]
    model_width = resid.shape[2]
    head_rows = model_width // seq_count
    experts_here = EXPERTS // seq_count
    chips = seq_count // CORES

    packed = jnp.concatenate([queries_keys[:, 0], values], axis=0)
    packed = packed.reshape(3, tokens, seq_count, head_rows).transpose(2, 0, 1, 3)
    heads = lax.all_to_all(packed, "seq", split_axis=0, concat_axis=0, tiled=True)
    queries = heads[:, 0].reshape(seq_count * tokens, head_rows)
    key_rows = heads[:, 1].reshape(seq_count * tokens, head_rows)
    value_rows = heads[:, 2].reshape(seq_count * tokens, head_rows)

    own_rows = lax.dynamic_slice_in_dim(out_weight, seq_index * head_rows, head_rows, axis=0)
    routes_meta = jnp.stack(
        [expert_ids.reshape(-1).astype(bf16), gate_vals.reshape(-1).astype(bf16)]
    )
    meta = jnp.pad(routes_meta, ((0, META_ROWS - 2), (0, 0)))
    spread = jnp.concatenate([own_rows, meta], axis=0)
    gathered = [spread] + [
        lax.ppermute(spread, "dp", ring_pairs(batch_count, -hop))
        for hop in range(1, batch_count)
    ]
    swap = [(i, i ^ 1) for i in range(batch_count)]
    gate_rows_t, up_rows_t, down_rows = expert_gate[0].T, expert_up[0].T, expert_down[0]
    middle = up_rows_t.shape[0] // 2
    own_gate, up_front = gate_rows_t, up_rows_t[:middle]
    other_gate = lax.ppermute(own_gate, "dp", swap)
    other_up_front = lax.ppermute(up_front, "dp", swap)

    attended = attend_heads(queries, key_rows, value_rows, doc_ids[0])
    gathered, attended = lax.optimization_barrier((gathered, attended))
    head_weight = columns_in_order(gathered, batch_index, head_rows)
    rolled_meta = [block[head_rows : head_rows + 2] for block in gathered]

    core = seq_index % CORES
    blocks = attended.reshape(chips, CORES * tokens * head_rows)
    blocks = lax.dynamic_slice_in_dim(
        jnp.concatenate([blocks, blocks], axis=0), seq_index // CORES, chips, axis=0
    ).reshape(chips, CORES, tokens, head_rows)
    own_blocks = lax.dynamic_index_in_dim(blocks, core, axis=1, keepdims=False)
    partner_blocks = lax.dynamic_index_in_dim(blocks, 1 - core, axis=1, keepdims=False)
    own_blocks = own_blocks.reshape(chips * tokens, head_rows)
    partner_blocks = partner_blocks.reshape(chips * tokens, head_rows)
    cores = [(i, i ^ 1) for i in range(seq_count)]
    width = model_width // PROJ_CHUNKS
    pieces = []
    for part in range(PROJ_CHUNKS):
        weight = head_weight[:, part * width : (part + 1) * width]
        crossed = lax.ppermute(dot(partner_blocks, weight).astype(bf16), "seq", cores)
        both = dot(own_blocks, weight) + crossed.astype(f32)
        both = both.reshape(chips, tokens, width)
        pieces.append(
            ring_scatter([both[j] for j in range(chips)], "seq", seq_count, CORES)
        )
    projected = jnp.concatenate(pieces, axis=1).astype(bf16)
    residual = (resid[0].astype(f32) + projected.astype(f32)).astype(bf16)
    stream = residual.astype(f32)
    normed = (
        stream * lax.rsqrt(jnp.mean(stream * stream, axis=-1, keepdims=True) + norm_eps) * norm_gain
    ).astype(bf16)

    even = batch_index % 2 == 0
    flat = tokens * TOPK
    served = batch_count // PAIR
    per_batch = served // BATCHES
    batch_tokens = per_batch * tokens
    routes_gates = jnp.stack(
        [rolled_meta[0]]
        + [
            jnp.where(even, rolled_meta[batch_count - hop], rolled_meta[hop])
            for hop in range(1, served)
        ]
    )
    routes = routes_gates[:, 0].astype(jnp.int32)
    order = jnp.arange(flat, dtype=jnp.int32)
    earlier = (routes[:, :, None] == routes[:, None, :]) & (order[None, :, None] > order[None, None, :])
    ranked = jnp.sum(earlier.astype(jnp.int32), axis=-1)
    place = jnp.arange(served, dtype=jnp.int32)[:, None] % per_batch
    rows_each = per_batch * CAP
    block_rows = HALVES * rows_each
    half_width = model_width // HALVES
    slot = jnp.where(
        routes % experts_here == batch_index // SPLIT,
        (routes // experts_here) * block_rows + place * CAP + ranked,
        -block_rows,
    ).reshape(served * tokens, TOPK)
    batch_rows = seq_count * rows_each
    row_range = jnp.arange(HALVES * batch_rows, dtype=jnp.int32)
    gate_rows = routes_gates[:, 1].reshape(served * tokens, TOPK)

    def pick_of(slots, batch):
        span = slice(batch * batch_tokens, (batch + 1) * batch_tokens)
        places = jnp.concatenate([slots[span] + h * rows_each for h in range(HALVES)], axis=0)
        return sum([(places[None, :, k] == row_range[:, None]).astype(bf16) for k in range(TOPK)])

    def combine_of(slots, batch):
        span = slice(batch * batch_tokens, (batch + 1) * batch_tokens)
        places = jnp.concatenate([slots[span] + h * rows_each for h in range(HALVES)], axis=0)
        gate_two = jnp.concatenate([gate_rows[span]] * HALVES, axis=0)
        return sum(
            [
                jnp.where(places[:, k, None] == row_range[None, :], gate_two[:, k, None], 0)
                for k in range(TOPK)
            ]
        ).astype(bf16)

    picks = [lax.optimization_barrier(pick_of(slot, 0))]

    half = batch_count // 2
    ahead, behind = {0: normed}, {0: normed}
    for hop in range(1, half):
        ahead[hop] = lax.ppermute(ahead[hop - 1], "dp", ring_pairs(batch_count, -1))
        behind[hop] = lax.ppermute(behind[hop - 1], "dp", ring_pairs(batch_count, 1))
    mine = [normed] + [
        lax.optimization_barrier(jnp.where(even, behind[hop], ahead[hop]))
        for hop in range(1, served)
    ]
    up_back, own_down, ahead[half - 1], behind[half - 1] = lax.optimization_barrier(
        (up_rows_t[middle:], down_rows, ahead[half - 1], behind[half - 1])
    )
    other_up_back = lax.ppermute(up_back, "dp", swap)
    other_down = lax.ppermute(own_down, "dp", swap)
    ahead[half] = lax.ppermute(ahead[half - 1], "dp", ring_pairs(batch_count, -1))
    other_up = jnp.concatenate([other_up_front, other_up_back], axis=0)

    def stack_halves(rows):
        return jnp.concatenate(
            [rows[:, h * half_width : (h + 1) * half_width] for h in range(HALVES)], axis=0
        )

    def along_seq(rows):
        return lax.all_to_all(
            rows.reshape(seq_count, block_rows, half_width),
            "seq",
            split_axis=0,
            concat_axis=0,
            tiled=True,
        ).reshape(HALVES * batch_rows, half_width)

    incoming = []
    for batch in range(BATCHES):
        block = jnp.concatenate(mine[batch * per_batch : (batch + 1) * per_batch], axis=0)
        outgoing = dot(picks[batch], stack_halves(block)).astype(bf16)
        if not batch:
            outgoing, slot = lax.optimization_barrier((outgoing, slot))
            picks.append(pick_of(slot, 1))
            by_device = row_range // block_rows * rows_each + row_range % rows_each
            by_half = row_range // rows_each % HALVES * batch_rows + by_device
            combines, to_half, to_device = lax.optimization_barrier(
                (
                    [combine_of(slot, i) for i in range(BATCHES)],
                    (by_half[None, :] == row_range[:, None]).astype(bf16),
                    (by_half[:, None] == row_range[None, :]).astype(bf16),
                )
            )
        if batch:
            outgoing, incoming[-1] = lax.optimization_barrier((outgoing, incoming[-1]))
        incoming.append(along_seq(outgoing))

    results = []
    for batch in range(BATCHES):
        results.append(
            expert_blocks(
                incoming[batch],
                to_half,
                to_device,
                (gate_rows_t, up_rows_t, down_rows),
                (other_gate, other_up, other_down),
            )
        )
    blocks = [ahead[j] for j in range(half + 1)] + [behind[j] for j in range(half - 1, 0, -1)]
    blocks, _ = lax.optimization_barrier((blocks, results[-1]))
    all_tokens = jnp.concatenate(blocks, axis=0)
    share_weight = jax.nn.sigmoid(dot(all_tokens, shared_score))
    shared_part = dot(hidden_of(all_tokens, shared_gate, shared_up), shared_down)
    shared_part = (shared_part * share_weight[:, None]).astype(bf16)

    results[0], _ = lax.optimization_barrier((results[0], shared_part))
    shared_part = shared_part.reshape(batch_count, tokens, model_width).astype(f32)

    routed = [None] * served
    last = None
    for batch in reversed(range(BATCHES)):
        rows = results[batch]
        if last is not None:
            rows, last = lax.optimization_barrier((rows, last))
        last = along_seq(rows)
        parts = dot(combines[batch], last).reshape(HALVES, per_batch, tokens, half_width)
        for i in range(per_batch):
            routed[batch * per_batch + i] = jnp.concatenate(
                [parts[h, i] for h in range(HALVES)], axis=1
            )

    def part_behind(hop):
        if hop < per_batch:
            return shared_part[batch_count - hop]
        return shared_part[batch_count - hop] + jnp.where(even, routed[hop], 0.0)

    def part_ahead(hop):
        if hop < per_batch:
            return shared_part[hop]
        return shared_part[hop] + jnp.where(even, 0.0, routed[hop])

    back = shared_part[half].astype(bf16)
    forth = part_ahead(half - 1).astype(bf16)
    for hop in range(half - 1, -1, -1):
        back = lax.ppermute(back, "dp", ring_pairs(batch_count, -1))
        if hop:
            back = (back.astype(f32) + part_behind(hop)).astype(bf16)
            forth = lax.ppermute(forth, "dp", ring_pairs(batch_count, 1))
        if hop > 1:
            forth = (forth.astype(f32) + part_ahead(hop - 1)).astype(bf16)
    towards = [(i, (i + (i % 2) * 2 - 1) % batch_count) for i in range(batch_count)]
    near = lax.ppermute(routed[1].astype(bf16), "dp", towards)
    layer_out = (
        residual.astype(f32)
        + routed[0]
        + shared_part[0]
        + back.astype(f32)
        + forth.astype(f32)
        + near.astype(f32)
    )
    return layer_out.astype(bf16)[None]


def solution(mesh):
    placed = (
        P(("groups", "dp"), "seq", None),
        P(None, ("groups", "dp"), "seq", None),
        P(("groups", "dp"), "seq", None),
        P(("groups", "dp"), None),
        P(None, "dp"),
        P(),
        P(("groups", "dp"), "seq", None),
        P(("groups", "dp"), "seq", None),
        P(("seq", "dp"), None, None),
        P(("seq", "dp"), None, None),
        P(("seq", "dp"), None, None),
        P(None, "dp"),
        P(None, "dp"),
        P("dp", None),
        P(),
    )
    return jax.shard_map(
        layer,
        mesh=mesh,
        in_specs=placed,
        out_specs=P(("groups", "dp"), "seq", None),
        check_vma=False,
    )
```

```python
import math

import jax
import jax.numpy as jnp
from jax import lax
from jax.experimental import pallas as pl
from jax.experimental.pallas import tpu as pltpu
from jax.sharding import PartitionSpec as P


EXPERTS = 32
TOPK = 4
SPLIT = 4
CAP = 10
PAIR = 2
CORES = 2
META_ROWS = 16
BATCHES = 2
PROJ_CHUNKS = 2
HALVES = 2
STEPS = 2


norm_eps = 1e-06
f32 = jnp.float32
bf16 = jnp.bfloat16


def dot(a, b):
    return jnp.dot(a, b, preferred_element_type=f32)


def attend_heads(queries, key_rows, value_rows, documents):
    score_scale = 1.0 / math.sqrt(queries.shape[-1])
    scores = (
        lax.dot_general(queries, key_rows, (((1,), (1,)), ((), ())), preferred_element_type=f32)
        * score_scale
    )
    positions = jnp.arange(queries.shape[0], dtype=jnp.int32)
    allowed = (positions[:, None] >= positions[None, :]) & (
        documents[:, None] == documents[None, :]
    )
    scores = jnp.where(allowed, scores, -1e30)
    row_max = jnp.max(scores, axis=-1, keepdims=True)
    lifted = jnp.exp(scores - row_max)
    weights = (lifted / jnp.sum(lifted, axis=-1, keepdims=True)).astype(bf16)
    return dot(weights, value_rows).astype(bf16)


def hidden_of(rows, gate_matrix, up_matrix):
    return (jax.nn.silu(dot(rows, gate_matrix)) * dot(rows, up_matrix)).astype(bf16)


def expert_kernel(x, to_half, to_device, go, uo, do, gx, ux, dx, y, rows, sums):
    step = pl.program_id(0)
    count, width = rows.shape[0], x.shape[1]

    @pl.when(step == 0)
    def _():
        for h in range(HALVES):
            rows[:, h * width : (h + 1) * width] = dot(
                to_half[h * count : (h + 1) * count, :], x[...]
            ).astype(bf16)

    def across(a, b):
        return lax.dot_general(a, b, (((1,), (1,)), ((), ())), preferred_element_type=f32)

    part = None
    for g, u, d in ((go, uo, do), (gx, ux, dx)):
        gate_act = across(rows[...], g[...])
        up_act = across(rows[...], u[...])
        hidden = (gate_act / (1.0 + jnp.exp(-gate_act)) * up_act).astype(bf16)
        out = dot(hidden, d[...])
        part = out if part is None else part + out

    @pl.when(step == 0)
    def _():
        sums[...] = part

    @pl.when(step > 0)
    def _():
        sums[...] = sums[...] + part

    @pl.when(step == pl.num_programs(0) - 1)
    def _():
        total = None
        for h in range(HALVES):
            out = sums[:, h * width : (h + 1) * width].astype(bf16)
            term = dot(to_device[:, h * count : (h + 1) * count], out)
            total = term if total is None else total + term
        y[...] = total.astype(bf16)


def expert_blocks(x, to_half, to_device, own, other):
    hidden, model_width = own[0].shape
    tile = hidden // STEPS
    count = x.shape[0] // HALVES
    whole = [pl.BlockSpec(a.shape, lambda j: (0, 0)) for a in (x, to_half, to_device)]
    tiled = [pl.BlockSpec((tile, model_width), lambda j: (j, 0))] * 6
    return pl.pallas_call(
        expert_kernel,
        grid=(STEPS,),
        in_specs=whole + tiled,
        out_specs=pl.BlockSpec(x.shape, lambda j: (0, 0)),
        out_shape=jax.ShapeDtypeStruct(x.shape, bf16),
        scratch_shapes=[
            pltpu.VMEM((count, model_width), bf16),
            pltpu.VMEM((count, model_width), f32),
        ],
        compiler_params=pltpu.CompilerParams(
            dimension_semantics=("arbitrary",), vmem_limit_bytes=60 << 20
        ),
        cost_estimate=pl.CostEstimate(
            flops=12 * count * hidden * model_width,
            bytes_accessed=12 * hidden * model_width,
            transcendentals=2 * count * hidden,
        ),
        name="expert_blocks",
    )(x, to_half, to_device, *own, *other)


def columns_kernel(starts, *refs):
    blocks, out = refs[:-1], refs[-1]
    width = blocks[0].shape[1]
    for j, block in enumerate(blocks):
        start = pl.multiple_of(starts[j], width)
        out[:, pl.ds(start, width)] = block[: out.shape[0], :]


def columns_in_order(blocks, first, rows):
    count, width = len(blocks), blocks[0].shape[1]
    starts = (first + jnp.arange(count, dtype=jnp.int32)) % count * width
    return pl.pallas_call(
        columns_kernel,
        in_specs=[pl.BlockSpec(memory_space=pltpu.SMEM)]
        + [pl.BlockSpec(memory_space=pltpu.VMEM)] * count,
        out_specs=pl.BlockSpec(memory_space=pltpu.VMEM),
        out_shape=jax.ShapeDtypeStruct((rows, count * width), bf16),
        name="columns_in_order",
    )(starts, *blocks)


def ring_pairs(size, step):
    return [(i, (i + step) % size) for i in range(size)]


def ring_scatter(parts, axis, size, step):
    forward, backward = ring_pairs(size, step), ring_pairs(size, -step)
    count = size // step
    half = count // 2
    left = parts[half].astype(bf16)
    right = parts[half - 1].astype(bf16)
    for hop in range(1, half + 1):
        left = lax.ppermute(left, axis, backward)
        if hop < half:
            left = (left.astype(f32) + parts[half + hop].astype(f32)).astype(bf16)
        if hop < half:
            right = lax.ppermute(right, axis, forward)
            if hop < half - 1:
                right = (right.astype(f32) + parts[half - 1 - hop].astype(f32)).astype(bf16)
    return parts[0].astype(f32) + left.astype(f32) + right.astype(f32)


def layer(
    resid,
    queries_keys,
    values,
    doc_ids,
    out_weight,
    norm_gain,
    expert_ids,
    gate_vals,
    expert_gate,
    expert_up,
    expert_down,
    shared_gate,
    shared_up,
    shared_down,
    shared_score,
):
    seq_count = lax.axis_size("seq")
    batch_count = lax.axis_size("dp")
    seq_index = lax.axis_index("seq")
    batch_index = lax.axis_index("dp")
    tokens = resid.shape[1]
    model_width = resid.shape[2]
    head_rows = model_width // seq_count
    experts_here = EXPERTS // seq_count
    chips = seq_count // CORES

    packed = jnp.concatenate([queries_keys[:, 0], values], axis=0)
    packed = packed.reshape(3, tokens, seq_count, head_rows).transpose(2, 0, 1, 3)
    heads = lax.all_to_all(packed, "seq", split_axis=0, concat_axis=0, tiled=True)
    queries = heads[:, 0].reshape(seq_count * tokens, head_rows)
    key_rows = heads[:, 1].reshape(seq_count * tokens, head_rows)
    value_rows = heads[:, 2].reshape(seq_count * tokens, head_rows)

    own_rows = lax.dynamic_slice_in_dim(out_weight, seq_index * head_rows, head_rows, axis=0)
    routes_meta = jnp.stack(
        [expert_ids.reshape(-1).astype(bf16), gate_vals.reshape(-1).astype(bf16)]
    )
    meta = jnp.pad(routes_meta, ((0, META_ROWS - 2), (0, 0)))
    spread = jnp.concatenate([own_rows, meta], axis=0)
    gathered = [spread] + [
        lax.ppermute(spread, "dp", ring_pairs(batch_count, -hop))
        for hop in range(1, batch_count)
    ]
    swap = [(i, i ^ 1) for i in range(batch_count)]
    gate_rows_t, up_rows_t, down_rows = expert_gate[0].T, expert_up[0].T, expert_down[0]
    middle = up_rows_t.shape[0] // 2
    own_gate, up_front = gate_rows_t, up_rows_t[:middle]
    other_gate = lax.ppermute(own_gate, "dp", swap)
    other_up_front = lax.ppermute(up_front, "dp", swap)

    attended = attend_heads(queries, key_rows, value_rows, doc_ids[0])
    gathered, attended = lax.optimization_barrier((gathered, attended))
    head_weight = columns_in_order(gathered, batch_index, head_rows)

    core = seq_index % CORES
    blocks = attended.reshape(chips, CORES * tokens * head_rows)
    blocks = lax.dynamic_slice_in_dim(
        jnp.concatenate([blocks, blocks], axis=0), seq_index // CORES, chips, axis=0
    ).reshape(chips, CORES, tokens, head_rows)
    own_blocks = lax.dynamic_index_in_dim(blocks, core, axis=1, keepdims=False)
    partner_blocks = lax.dynamic_index_in_dim(blocks, 1 - core, axis=1, keepdims=False)
    own_blocks = own_blocks.reshape(chips * tokens, head_rows)
    partner_blocks = partner_blocks.reshape(chips * tokens, head_rows)
    own_blocks, partner_blocks = lax.optimization_barrier((own_blocks, partner_blocks))
    cores = [(i, i ^ 1) for i in range(seq_count)]
    crossed = lax.ppermute(partner_blocks, "seq", cores)
    other_weight = lax.ppermute(head_weight, "seq", cores)
    width = model_width // PROJ_CHUNKS
    pieces = []
    for part in range(PROJ_CHUNKS):
        cut = slice(part * width, (part + 1) * width)
        both = dot(own_blocks, head_weight[:, cut]) + dot(crossed, other_weight[:, cut])
        both = both.reshape(chips, tokens, width)
        pieces.append(
            ring_scatter([both[j] for j in range(chips)], "seq", seq_count, CORES)
        )
    projected = jnp.concatenate(pieces, axis=1).astype(bf16)
    gathered, projected = lax.optimization_barrier((gathered, projected))
    rolled_meta = [block[head_rows : head_rows + 2] for block in gathered]
    residual = (resid[0].astype(f32) + projected.astype(f32)).astype(bf16)
    stream = residual.astype(f32)
    normed = (
        stream * lax.rsqrt(jnp.mean(stream * stream, axis=-1, keepdims=True) + norm_eps) * norm_gain
    ).astype(bf16)

    even = batch_index % 2 == 0
    flat = tokens * TOPK
    served = batch_count // PAIR
    per_batch = served // BATCHES
    batch_tokens = per_batch * tokens
    routes_gates = jnp.stack(
        [rolled_meta[0]]
        + [
            jnp.where(even, rolled_meta[batch_count - hop], rolled_meta[hop])
            for hop in range(1, served)
        ]
    )
    routes = routes_gates[:, 0].astype(jnp.int32)
    order = jnp.arange(flat, dtype=jnp.int32)
    earlier = (routes[:, :, None] == routes[:, None, :]) & (order[None, :, None] > order[None, None, :])
    ranked = jnp.sum(earlier.astype(jnp.int32), axis=-1)
    place = jnp.arange(served, dtype=jnp.int32)[:, None] % per_batch
    rows_each = per_batch * CAP
    block_rows = HALVES * rows_each
    half_width = model_width // HALVES
    slot = jnp.where(
        routes % experts_here == batch_index // SPLIT,
        (routes // experts_here) * block_rows + place * CAP + ranked,
        -block_rows,
    ).reshape(served * tokens, TOPK)
    batch_rows = seq_count * rows_each
    row_range = jnp.arange(HALVES * batch_rows, dtype=jnp.int32)
    gate_rows = routes_gates[:, 1].reshape(served * tokens, TOPK)

    def pick_of(slots, batch):
        span = slice(batch * batch_tokens, (batch + 1) * batch_tokens)
        places = jnp.concatenate([slots[span] + h * rows_each for h in range(HALVES)], axis=0)
        return sum([(places[None, :, k] == row_range[:, None]).astype(bf16) for k in range(TOPK)])

    def combine_of(slots, batch):
        span = slice(batch * batch_tokens, (batch + 1) * batch_tokens)
        places = jnp.concatenate([slots[span] + h * rows_each for h in range(HALVES)], axis=0)
        gate_two = jnp.concatenate([gate_rows[span]] * HALVES, axis=0)
        return sum(
            [
                jnp.where(places[:, k, None] == row_range[None, :], gate_two[:, k, None], 0)
                for k in range(TOPK)
            ]
        ).astype(bf16)

    picks = [lax.optimization_barrier(pick_of(slot, 0))]

    half = batch_count // 2
    ahead, behind = {0: normed}, {0: normed}
    for hop in range(1, half):
        ahead[hop] = lax.ppermute(ahead[hop - 1], "dp", ring_pairs(batch_count, -1))
        behind[hop] = lax.ppermute(behind[hop - 1], "dp", ring_pairs(batch_count, 1))
    mine = [normed] + [
        lax.optimization_barrier(jnp.where(even, behind[hop], ahead[hop]))
        for hop in range(1, served)
    ]
    up_back, own_down, ahead[half - 1], behind[half - 1] = lax.optimization_barrier(
        (up_rows_t[middle:], down_rows, ahead[half - 1], behind[half - 1])
    )
    other_up_back = lax.ppermute(up_back, "dp", swap)
    other_down = lax.ppermute(own_down, "dp", swap)
    ahead[half] = lax.ppermute(ahead[half - 1], "dp", ring_pairs(batch_count, -1))
    other_up = jnp.concatenate([other_up_front, other_up_back], axis=0)

    def stack_halves(rows):
        return jnp.concatenate(
            [rows[:, h * half_width : (h + 1) * half_width] for h in range(HALVES)], axis=0
        )

    def along_seq(rows):
        return lax.all_to_all(
            rows.reshape(seq_count, block_rows, half_width),
            "seq",
            split_axis=0,
            concat_axis=0,
            tiled=True,
        ).reshape(HALVES * batch_rows, half_width)

    incoming = []
    for batch in range(BATCHES):
        block = jnp.concatenate(mine[batch * per_batch : (batch + 1) * per_batch], axis=0)
        outgoing = dot(picks[batch], stack_halves(block)).astype(bf16)
        if not batch:
            outgoing, slot = lax.optimization_barrier((outgoing, slot))
            picks.append(pick_of(slot, 1))
            by_device = row_range // block_rows * rows_each + row_range % rows_each
            by_half = row_range // rows_each % HALVES * batch_rows + by_device
            combines, to_half, to_device = lax.optimization_barrier(
                (
                    [combine_of(slot, i) for i in range(BATCHES)],
                    (by_half[None, :] == row_range[:, None]).astype(bf16),
                    (by_half[:, None] == row_range[None, :]).astype(bf16),
                )
            )
        if batch:
            outgoing, incoming[-1] = lax.optimization_barrier((outgoing, incoming[-1]))
        incoming.append(along_seq(outgoing))

    results = []
    for batch in range(BATCHES):
        results.append(
            expert_blocks(
                incoming[batch],
                to_half,
                to_device,
                (gate_rows_t, up_rows_t, down_rows),
                (other_gate, other_up, other_down),
            )
        )
    blocks = [ahead[j] for j in range(half + 1)] + [behind[j] for j in range(half - 1, 0, -1)]
    blocks, _ = lax.optimization_barrier((blocks, results[-1]))
    all_tokens = jnp.concatenate(blocks, axis=0)
    share_weight = jax.nn.sigmoid(dot(all_tokens, shared_score))
    shared_part = dot(hidden_of(all_tokens, shared_gate, shared_up), shared_down)
    shared_part = (shared_part * share_weight[:, None]).astype(bf16)

    results[0], _ = lax.optimization_barrier((results[0], shared_part))
    shared_part = shared_part.reshape(batch_count, tokens, model_width).astype(f32)

    routed = [None] * served
    last = None
    for batch in reversed(range(BATCHES)):
        rows = results[batch]
        if last is not None:
            rows, last = lax.optimization_barrier((rows, last))
        last = along_seq(rows)
        parts = dot(combines[batch], last).reshape(HALVES, per_batch, tokens, half_width)
        for i in range(per_batch):
            routed[batch * per_batch + i] = jnp.concatenate(
                [parts[h, i] for h in range(HALVES)], axis=1
            )

    def part_behind(hop):
        if hop < per_batch:
            return shared_part[batch_count - hop]
        return shared_part[batch_count - hop] + jnp.where(even, routed[hop], 0.0)

    def part_ahead(hop):
        if hop < per_batch:
            return shared_part[hop]
        return shared_part[hop] + jnp.where(even, 0.0, routed[hop])

    back = shared_part[half].astype(bf16)
    forth = part_ahead(half - 1).astype(bf16)
    for hop in range(half - 1, -1, -1):
        back = lax.ppermute(back, "dp", ring_pairs(batch_count, -1))
        if hop:
            back = (back.astype(f32) + part_behind(hop)).astype(bf16)
            forth = lax.ppermute(forth, "dp", ring_pairs(batch_count, 1))
        if hop > 1:
            forth = (forth.astype(f32) + part_ahead(hop - 1)).astype(bf16)
    towards = [(i, (i + (i % 2) * 2 - 1) % batch_count) for i in range(batch_count)]
    near = lax.ppermute(routed[1].astype(bf16), "dp", towards)
    layer_out = (
        residual.astype(f32)
        + routed[0]
        + shared_part[0]
        + back.astype(f32)
        + forth.astype(f32)
        + near.astype(f32)
    )
    return layer_out.astype(bf16)[None]


def solution(mesh):
    placed = (
        P(("groups", "dp"), "seq", None),
        P(None, ("groups", "dp"), "seq", None),
        P(("groups", "dp"), "seq", None),
        P(("groups", "dp"), None),
        P(None, "dp"),
        P(),
        P(("groups", "dp"), "seq", None),
        P(("groups", "dp"), "seq", None),
        P(("seq", "dp"), None, None),
        P(("seq", "dp"), None, None),
        P(("seq", "dp"), None, None),
        P(None, "dp"),
        P(None, "dp"),
        P("dp", None),
        P(),
    )
    return jax.shard_map(
        layer,
        mesh=mesh,
        in_specs=placed,
        out_specs=P(("groups", "dp"), "seq", None),
        check_vma=False,
    )
```
